32 devices in a mesh: tensor: 2 (over y), dp: 4 (over x, core), seq: 4 (over z).
Axes of the slice: x: 2, y: 2, z: 4, core: 2. Of those that a mesh axis runs over, the one named last changes fastest.
Arguments:
- tokens: bfloat16 [8, 1024, 2048], P('dp', 'seq'), may hold values from -6 to 6
- ln1_gain: bfloat16 [2048], P(('dp', 'seq')), may hold values from 0.5 to 1.5
- ln1_bias: bfloat16 [2048], P(('dp', 'seq')), may hold values from -3 to 3
- ln2_gain: bfloat16 [2048], P(('dp', 'seq')), may hold values from 0.5 to 1.5
- ln2_bias: bfloat16 [2048], P(('dp', 'seq')), may hold values from -3 to 3
- w_query: bfloat16 [2048, 2048], P(('dp', 'seq'), 'tensor'), may hold values from -0.125 to 0.125
- w_key: bfloat16 [2048, 2048], P(('dp', 'seq'), 'tensor'), may hold values from -0.125 to 0.125
- w_value: bfloat16 [2048, 4096], P(('dp', 'seq'), 'tensor'), may hold values from -0.125 to 0.125
- w_swish: bfloat16 [2048, 4096], P(('dp', 'seq'), 'tensor'), may hold values from -0.125 to 0.125
- w_out: bfloat16 [4096, 2048], P('tensor', ('dp', 'seq')), may hold values from -0.1875 to 0.1875
- w_gate: bfloat16 [2048, 4096], P(('dp', 'seq'), 'tensor'), may hold values from -0.125 to 0.125
- w_up: bfloat16 [2048, 4096], P(('dp', 'seq'), 'tensor'), may hold values from -0.125 to 0.125
- w_down: bfloat16 [4096, 2048], P('tensor', ('dp', 'seq')), may hold values from -0.09375 to 0.09375
- decay_rate: float32 [8], P('tensor'), may hold values from 0 to 1, as said below
- cotangent: bfloat16 [8, 1024, 2048], P('dp', 'seq'), may hold values from -6 to 6
Outputs:
- mixed_out: bfloat16 [8, 1024, 2048], P('dp', 'seq')
- input_grad: float32 [8, 1024, 2048], P('dp', 'seq')
- ln1_gain_grad: float32 [2048], P(('dp', 'seq'))
- ln1_bias_grad: float32 [2048], P(('dp', 'seq'))
- ln2_gain_grad: float32 [2048], P(('dp', 'seq'))
- ln2_bias_grad: float32 [2048], P(('dp', 'seq'))
- w_query_grad: float32 [2048, 2048], P(('dp', 'seq'), 'tensor')
- w_key_grad: float32 [2048, 2048], P(('dp', 'seq'), 'tensor')
- w_value_grad: float32 [2048, 4096], P(('dp', 'seq'), 'tensor')
- w_swish_grad: float32 [2048, 4096], P(('dp', 'seq'), 'tensor')
- w_out_grad: float32 [4096, 2048], P('tensor', ('dp', 'seq'))
- w_gate_grad: float32 [2048, 4096], P(('dp', 'seq'), 'tensor')
- w_up_grad: float32 [2048, 4096], P(('dp', 'seq'), 'tensor')
- w_down_grad: float32 [4096, 2048], P('tensor', ('dp', 'seq'))
The draws below stay inside these ranges and needn't reach their ends.
Inputs may be any that keep to these rules, and one draw needn't show every extreme that they name: `decay_rate`: each head's rate lies between 0.3 / 1024 and 1 / 30.
All inputs are finite; a program needn't handle non-finite values.
Results may differ from the reference program's by a relative error of at most 0.014.
Values may be sent and summed in bfloat16 or wider, within the bound.
A program may use at most 256 MiB of HBM per device.

```python
import jax
import jax.numpy as jnp
from jax import lax

D = 2048
HEADS = 8
KD = 256
VH = 512
FF = 4096
TB = 256
LENGTH = 1024
BATCH = 8


def draw_decay_rate(key, part):
    picker, slow_key, fast_key = jax.random.split(jax.random.fold_in(key, 7), 3)
    order = jax.random.permutation(picker, HEADS)
    slow_count = HEADS // 2
    slow_rates = jnp.exp(jax.random.uniform(slow_key, (HEADS,), jnp.float32, jnp.log(0.3 / LENGTH), jnp.log(2.0 / LENGTH)))
    fast_rates = jnp.exp(jax.random.uniform(fast_key, (HEADS,), jnp.float32, jnp.log(1.0 / 50.0), jnp.log(1.0 / 30.0)))
    return jnp.where(order < slow_count, slow_rates, fast_rates).astype(jnp.float32)


def block_scale(key, dims, cuts, least, largest):
    def one(axis_at, parts):
        steps = jax.random.uniform(jax.random.fold_in(jax.random.fold_in(key, 6), axis_at), (parts,), jnp.float32, least / len(cuts), largest / len(cuts))
        return jnp.repeat(jnp.exp(steps), dims[axis_at] // parts).reshape((-1,) + (1,) * (len(dims) - axis_at - 1))

    gain = one(*cuts[0])
    for cut in cuts[1:]:
        gain = gain * one(*cut)
    return gain


def gaussian(rng, dims, scale, bound, shards=(), held_as=jnp.bfloat16):
    level = block_scale(rng, dims, shards, -0.22, 0.18) if shards else 1.0
    values = jax.random.normal(rng, dims, jnp.float32) * scale * level
    return jnp.minimum(jnp.maximum(values, -bound), bound).astype(held_as)


def setup_inputs(seed: int = 0) -> dict:
    seeds = jax.random.split(jax.random.key(seed), 16)
    tokens = gaussian(seeds[0], (BATCH, LENGTH, D), 1.0, 6.0, ((0, 4), (1, 4)))
    ln1_gain = jnp.clip(1.0 + 0.1 * jax.random.normal(seeds[1], (D,), jnp.float32), 0.5, 1.5).astype(jnp.bfloat16)
    ln1_bias = gaussian(seeds[2], (D,), 0.5, 3.0, ((0, 16),))
    ln2_gain = jnp.clip(1.0 + 0.1 * jax.random.normal(seeds[3], (D,), jnp.float32), 0.5, 1.5).astype(jnp.bfloat16)
    ln2_bias = gaussian(seeds[4], (D,), 0.5, 3.0, ((0, 16),))
    w_query = gaussian(seeds[5], (D, HEADS * KD), D ** -0.5, 0.125, ((0, 16), (1, 2)))
    w_key = gaussian(seeds[6], (D, HEADS * KD), D ** -0.5, 0.125, ((0, 16), (1, 2)))
    w_value = gaussian(seeds[7], (D, HEADS * VH), D ** -0.5, 0.125, ((0, 16), (1, 2)))
    w_swish = gaussian(seeds[8], (D, HEADS * VH), D ** -0.5, 0.125, ((0, 16), (1, 2)))
    w_out = gaussian(seeds[9], (HEADS * VH, D), (HEADS * VH // 4) ** -0.5, 0.1875, ((0, 2), (1, 16)))
    w_gate = gaussian(seeds[10], (D, FF), D ** -0.5, 0.125, ((0, 16), (1, 2)))
    w_up = gaussian(seeds[11], (D, FF), D ** -0.5, 0.125, ((0, 16), (1, 2)))
    w_down = gaussian(seeds[12], (FF, D), FF ** -0.5, 0.09375, ((0, 2), (1, 16)))
    decay_rate = draw_decay_rate(jax.random.fold_in(seeds[15], 71), 0)
    cotangent = gaussian(seeds[14], (BATCH, LENGTH, D), 1.0, 6.0, ((0, 4), (1, 4)))
    return {"tokens": tokens, "ln1_gain": ln1_gain, "ln1_bias": ln1_bias, "ln2_gain": ln2_gain, "ln2_bias": ln2_bias, "w_query": w_query, "w_key": w_key, "w_value": w_value, "w_swish": w_swish, "w_out": w_out, "w_gate": w_gate, "w_up": w_up, "w_down": w_down, "decay_rate": decay_rate, "cotangent": cotangent}


eps = 1e-05
highest_precision = lax.Precision.HIGHEST

@jax.custom_vjp
def low(v):
    return lax.optimization_barrier(v.astype(jnp.bfloat16)).astype(jnp.float32)

@jax.custom_vjp
def low_back(v):
    return v

def low_keep(v):
    return (low(v), None)

def low_pass(kept, grad):
    return (grad,)

def back_keep(v):
    return (v, None)

def back_low(kept, grad):
    return (low(grad),)
low.defvjp(low_keep, low_pass)
low_back.defvjp(back_keep, back_low)

def normalize(values):
    centred = values - lax.optimization_barrier(jnp.mean(values, axis=-1, keepdims=True))
    spread = lax.optimization_barrier(jnp.mean(centred * centred, axis=-1, keepdims=True))
    return centred * lax.rsqrt(spread + eps)

def turn_angles(positions, half_width):
    frequency = 10000.0 ** (-jnp.arange(half_width, dtype=jnp.float32) / max(half_width - 1, 1))
    angles = positions[:, None] * frequency[None, :]
    return (jnp.cos(angles)[:, None, :], jnp.sin(angles)[:, None, :])

def rotate(values, cosine, sine_table):
    half_width = values.shape[-1] // 2
    first_half = values[..., :half_width]
    second_half = values[..., half_width:]
    return jnp.concatenate([first_half * cosine - second_half * sine_table, second_half * cosine + first_half * sine_table], axis=-1)

def decay_tables(decay_rate, block):
    places = jnp.arange(block, dtype=jnp.float32)
    distance = places[:, None] - places[None, :]
    inside = jnp.where(distance[None] >= 0.0, jnp.exp(-decay_rate[:, None, None] * jnp.maximum(distance, 0.0)[None]), 0.0)
    query_decay_factor = jnp.exp(-decay_rate[None, :] * (places[:, None] + 1.0))[..., None]
    key_decay_factor = jnp.exp(-decay_rate[None, :] * (block - 1.0 - places[:, None]))[..., None]
    block_decay_factor = jnp.exp(-decay_rate * block)[:, None, None]
    return (inside, query_decay_factor, key_decay_factor, block_decay_factor)

def retention(query_rot, key_rot, value_rows, decay_rate):
    inside, query_decay_factor, key_decay_factor, block_decay_factor = decay_tables(decay_rate, TB)
    length = query_rot.shape[0]
    blocks = length // TB

    def advance(carried_state, pieces):
        query_block, key_block, value_block = pieces
        scores = low_back(jnp.einsum('nhk,mhk->hnm', query_block, key_block, precision=highest_precision))
        weights = low(scores * inside)
        within = jnp.einsum('hnm,mhv->nhv', weights, value_block, precision=highest_precision)
        cross_block_term = jnp.einsum('dpz,pza->dpa', query_block * query_decay_factor, carried_state, precision=highest_precision)
        updated_state = carried_state * block_decay_factor + jnp.einsum('glf,glz->lfz', key_block * key_decay_factor, value_block, precision=highest_precision)
        return (updated_state, within + cross_block_term)
    initial = jnp.zeros((HEADS, KD, VH), jnp.float32)
    shaped = (query_rot.reshape(blocks, TB, HEADS, KD), key_rot.reshape(blocks, TB, HEADS, KD), value_rows.reshape(blocks, TB, HEADS, VH))
    ending, outputs = lax.scan(jax.checkpoint(advance), initial, shaped)
    return outputs.reshape(length, HEADS, VH)

def reference(tokens, ln1_gain, ln1_bias, ln2_gain, ln2_bias, w_query, w_key, w_value, w_swish, w_out, w_gate, w_up, w_down, decay_rate, cotangent):
    weights = tuple((matrix.astype(jnp.float32) for matrix in (ln1_gain, ln1_bias, ln2_gain, ln2_bias, w_query, w_key, w_value, w_swish, w_out, w_gate, w_up, w_down)))
    positions = jnp.arange(LENGTH, dtype=jnp.float32)
    cosine, sine_table = turn_angles(positions, KD // 2)
    rates = decay_rate.astype(jnp.float32)

    def layer(inputs, norm_gain, norm_bias, mlp_gain, mlp_bias, query_w, key_w, value_w, swish_w, out_w, gate_w, up_w, down_w):
        length = inputs.shape[0]
        first = low(normalize(inputs) * norm_gain + norm_bias)
        queries = low_back(jnp.dot(first, query_w, precision=highest_precision)).reshape(length, HEADS, KD)
        keys_lin = low_back(jnp.dot(first, key_w, precision=highest_precision)).reshape(length, HEADS, KD)
        value_rows = low(low_back(jnp.dot(first, value_w, precision=highest_precision))).reshape(length, HEADS, VH)
        gate_pre = low_back(jnp.dot(first, swish_w, precision=highest_precision))
        query_rot = low(rotate(queries, cosine, sine_table))
        key_rot = low(rotate(keys_lin, cosine, sine_table))
        retained = low_back(retention(query_rot, key_rot, value_rows, rates))
        group_flat = normalize(retained).reshape(length, HEADS * VH)
        mixed = low(jax.nn.silu(gate_pre) * group_flat)
        hidden_in = inputs + low_back(jnp.dot(mixed, out_w, precision=highest_precision))
        second = low(normalize(hidden_in) * mlp_gain + mlp_bias)
        gate_lin = low_back(jnp.dot(second, gate_w, precision=highest_precision))
        up_lin = low_back(jnp.dot(second, up_w, precision=highest_precision))
        hidden = low(jax.nn.gelu(gate_lin) * up_lin)
        return hidden_in + low_back(jnp.dot(hidden, down_w, precision=highest_precision))

    def per_sequence(totals, couple):
        inputs, grads_out = couple
        result, pullback = jax.vjp(layer, inputs.astype(jnp.float32), *weights)
        gradients = pullback(grads_out.astype(jnp.float32))
        totals = tuple((total + piece for total, piece in zip(totals, gradients[1:])))
        return (totals, (result.astype(jnp.bfloat16), gradients[0]))
    zeros = tuple((jnp.zeros(matrix.shape, jnp.float32) for matrix in weights))
    totals, (mixed_out, input_grad) = lax.scan(per_sequence, zeros, (tokens, cotangent))
    return (mixed_out, input_grad, totals[0], totals[1], totals[2], totals[3], totals[4], totals[5], totals[6], totals[7], totals[8], totals[9], totals[10], totals[11])
```

```python
import jax
import jax.numpy as jnp
from jax import lax
from jax.sharding import PartitionSpec as P

KD = 256
VH = 512
GROUP = ("dp", "seq")

eps = 1e-05


def normalize(values):
    centred = values - jnp.mean(values, axis=-1, keepdims=True)
    spread = jnp.mean(centred * centred, axis=-1, keepdims=True)
    scaling = lax.rsqrt(spread + eps)
    return (centred * scaling, scaling)


def norm_back(grad_normed, normed, scaling):
    first_mean = jnp.mean(grad_normed, axis=-1, keepdims=True)
    second_mean = jnp.mean(grad_normed * normed, axis=-1, keepdims=True)
    return scaling * (grad_normed - first_mean - normed * second_mean)


def turn_angles(positions, half_width):
    frequency = 10000.0 ** (-jnp.arange(half_width, dtype=jnp.float32) / max(half_width - 1, 1))
    angles = positions[:, None] * frequency[None, :]
    return (jnp.cos(angles)[:, None, :], jnp.sin(angles)[:, None, :])


def rotate(values, cosine, sine_table):
    half_width = values.shape[-1] // 2
    first_half = values[..., :half_width]
    second_half = values[..., half_width:]
    return jnp.concatenate(
        [
            first_half * cosine - second_half * sine_table,
            second_half * cosine + first_half * sine_table,
        ],
        axis=-1,
    )


def decay_tables(decay_rate, block):
    places = jnp.arange(block, dtype=jnp.float32)
    distance = places[:, None] - places[None, :]
    inside = jnp.where(
        distance[None] >= 0.0,
        jnp.exp(-decay_rate[:, None, None] * jnp.maximum(distance, 0.0)[None]),
        0.0,
    )
    query_decay_factor = jnp.exp(-decay_rate[None, :] * (places[:, None] + 1.0))[..., None]
    key_decay_factor = jnp.exp(-decay_rate[None, :] * (block - 1.0 - places[:, None]))[..., None]
    block_decay_factor = jnp.exp(-decay_rate * block)[:, None, None]
    return (inside, query_decay_factor, key_decay_factor, block_decay_factor)


def f32_einsum(spec, left, right):
    return jnp.einsum(spec, left, right, preferred_element_type=jnp.float32)


def low(values):
    return values.astype(jnp.bfloat16)


def wide(values):
    return values.astype(jnp.float32)


def gather_rows(shard):
    return lax.all_gather(shard, GROUP, axis=0, tiled=True)


def scatter_rows(partial):
    return lax.psum_scatter(partial, GROUP, scatter_dimension=0, tiled=True).astype(jnp.float32)


def tensor_sum(partial):
    if lax.axis_size("tensor") != 2:
        return lax.psum(partial, "tensor")
    mine = low(partial)
    other = lax.ppermute(mine, "tensor", [(0, 1), (1, 0)])
    return wide(mine) + wide(other)


def group_sum(partial):
    for axis in GROUP:
        count = lax.axis_size(axis)
        stride = 1
        while stride < count:
            partial = partial + lax.ppermute(
                partial, axis, [(i, i ^ stride) for i in range(count)]
            )
            stride *= 2
    return partial


def along_sequence(local, decay, forward):
    count = lax.axis_size("seq")
    pieces = local.shape[1] if count <= 4 else 1
    width = local.shape[1] // pieces
    entering = []
    for piece in range(pieces):
        own = local[:, piece * width : (piece + 1) * width]
        rate = decay[piece * width : (piece + 1) * width]
        got = jnp.zeros(own.shape, jnp.bfloat16)
        for turn in range(count - 1):
            pair = (turn, turn + 1) if forward else (count - 1 - turn, count - 2 - turn)
            leaving = low(rate * wide(got) + own)
            got = got + lax.ppermute(leaving, "seq", [pair])
        entering.append(got)
    return jnp.concatenate(entering, axis=1)


def on_device(
    tokens,
    ln1_gain,
    ln1_bias,
    ln2_gain,
    ln2_bias,
    w_query,
    w_key,
    w_value,
    w_swish,
    w_out,
    w_gate,
    w_up,
    w_down,
    decay_rate,
    cotangent,
):
    seq_count, block, width = tokens.shape
    row_count = seq_count * block
    heads = decay_rate.shape[0]
    keys = heads * KD
    values = heads * VH
    units = w_gate.shape[1]
    small = jnp.stack([ln1_gain, ln1_bias, ln2_gain, ln2_bias], axis=1)
    small = jnp.pad(small, ((0, 0), (0, 124)))
    front = gather_rows(jnp.concatenate([w_query, w_key, w_value, w_swish, small], axis=1))
    out_full = gather_rows(w_out.T)
    ffn = gather_rows(jnp.concatenate([w_gate, w_up, w_down.T], axis=1))
    front_w = front[:, : 2 * keys + 2 * values]
    vectors = wide(front[:, 2 * keys + 2 * values : 2 * keys + 2 * values + 4]).T
    norm_gain, norm_bias, mlp_gain, mlp_bias = vectors[0], vectors[1], vectors[2], vectors[3]
    up_w = ffn[:, : 2 * units]
    down_w = ffn[:, 2 * units :]

    inputs = wide(tokens).reshape(row_count, width)
    normed_one, scale_one = normalize(inputs)
    first = low(normed_one * norm_gain + norm_bias)
    projected = f32_einsum("rd,dk->rk", first, front_w)
    queries = projected[:, :keys].reshape(seq_count, block, heads, KD)
    keys_lin = projected[:, keys : 2 * keys].reshape(seq_count, block, heads, KD)
    value_rows = low(projected[:, 2 * keys : 2 * keys + values]).reshape(
        seq_count, block, heads, VH
    )
    gate_pre = projected[:, 2 * keys + values :]
    offset = lax.axis_index("seq") * block
    positions = wide(offset + jnp.arange(block, dtype=jnp.int32))
    cosine, sine_table = turn_angles(positions, KD // 2)
    query_rot = low(rotate(queries, cosine, sine_table))
    key_rot = low(rotate(keys_lin, cosine, sine_table))
    inside, query_decay, key_decay, block_decay = decay_tables(decay_rate, block)
    query_scaled = low(wide(query_rot) * query_decay)
    key_scaled = low(wide(key_rot) * key_decay)
    local_state = f32_einsum("smhk,smhv->shkv", key_scaled, value_rows)
    state_in = along_sequence(local_state, block_decay, True)
    scores = f32_einsum("snhk,smhk->shnm", query_rot, key_rot)
    weights = low(scores * inside)
    within = f32_einsum("shnm,smhv->snhv", weights, value_rows)
    retained = within + f32_einsum("snhk,shkv->snhv", query_scaled, state_in)
    group_normed, group_scale = normalize(retained)
    group_flat = group_normed.reshape(row_count, values)
    gate_act, swish_pull = jax.vjp(jax.nn.silu, gate_pre)
    mixed = low(gate_act * group_flat)
    hidden_in = inputs + tensor_sum(f32_einsum("rv,dv->rd", mixed, out_full))
    normed_two, scale_two = normalize(hidden_in)
    second = low(normed_two * mlp_gain + mlp_bias)
    lin = f32_einsum("rd,df->rf", second, up_w)
    gate_lin = lin[:, :units]
    up_lin = lin[:, units:]
    gate_gelu, gelu_pull = jax.vjp(jax.nn.gelu, gate_lin)
    hidden = low(gate_gelu * up_lin)
    mixed_out = low(hidden_in + tensor_sum(f32_einsum("rf,df->rd", hidden, down_w)))
    mixed_out = mixed_out.reshape(seq_count, block, width)

    grad_rows = cotangent.reshape(row_count, width)
    grad_down = low(f32_einsum("rd,rf->df", grad_rows, hidden))
    grad_hidden = f32_einsum("rd,df->rf", grad_rows, down_w)
    grad_lin = jnp.concatenate(
        [low(gelu_pull(grad_hidden * up_lin)[0]), low(grad_hidden * gate_gelu)], axis=1
    )
    grad_up = low(f32_einsum("rd,rf->df", second, grad_lin))
    grad_second = tensor_sum(f32_einsum("rf,df->rd", grad_lin, up_w))
    grad_mlp_gain = jnp.sum(grad_second * normed_two, axis=0)
    grad_mlp_bias = jnp.sum(grad_second, axis=0)
    grad_hidden_in = wide(grad_rows) + norm_back(grad_second * mlp_gain, normed_two, scale_two)
    grad_branch = low(grad_hidden_in)
    grad_out = low(f32_einsum("rd,rv->dv", grad_branch, mixed))
    grad_mixed = f32_einsum("rd,dv->rv", grad_branch, out_full)
    grad_gate_pre = low(swish_pull(grad_mixed * group_flat)[0])
    grad_group = (grad_mixed * gate_act).reshape(seq_count, block, heads, VH)
    grad_retained = low(norm_back(grad_group, group_normed, group_scale))
    local_grad = f32_einsum("snhk,snhv->shkv", query_scaled, grad_retained)
    state_grad = along_sequence(local_grad, block_decay, False)
    grad_weights = f32_einsum("snhv,smhv->shnm", grad_retained, value_rows)
    grad_scores = low(grad_weights * inside)
    grad_query = f32_einsum("shnm,smhk->snhk", grad_scores, key_rot)
    grad_query = grad_query + query_decay * f32_einsum(
        "snhv,shkv->snhk", grad_retained, state_in
    )
    grad_key = f32_einsum("shnm,snhk->smhk", grad_scores, query_rot)
    grad_key = grad_key + key_decay * f32_einsum("smhv,shkv->smhk", value_rows, state_grad)
    grad_value = f32_einsum("shnm,snhv->smhv", weights, grad_retained)
    grad_value = grad_value + f32_einsum("smhk,shkv->smhv", key_scaled, state_grad)
    grad_query_pre = low(rotate(grad_query, cosine, -sine_table)).reshape(row_count, keys)
    grad_key_pre = low(rotate(grad_key, cosine, -sine_table)).reshape(row_count, keys)
    grad_value_pre = low(grad_value).reshape(row_count, values)
    grad_projected = jnp.concatenate(
        [grad_query_pre, grad_key_pre, grad_value_pre, grad_gate_pre], axis=1
    )
    grad_front = low(f32_einsum("rd,rk->dk", first, grad_projected))
    grad_first = tensor_sum(f32_einsum("rk,dk->rd", grad_projected, front_w))
    grad_norm_gain = jnp.sum(grad_first * normed_one, axis=0)
    grad_norm_bias = jnp.sum(grad_first, axis=0)
    grad_inputs = grad_hidden_in + norm_back(grad_first * norm_gain, normed_one, scale_one)
    input_grad = grad_inputs.reshape(seq_count, block, width)

    down_sum = scatter_rows(grad_down).T
    up_sum = scatter_rows(grad_up)
    out_sum = scatter_rows(grad_out).T
    front_sum = scatter_rows(grad_front)
    vector_sums = group_sum(
        jnp.stack([grad_norm_gain, grad_norm_bias, grad_mlp_gain, grad_mlp_bias])
    )
    shard = ln1_gain.shape[0]
    vector_sums = lax.dynamic_slice_in_dim(
        vector_sums, lax.axis_index(GROUP) * shard, shard, axis=1
    )
    return (
        mixed_out,
        input_grad,
        vector_sums[0],
        vector_sums[1],
        vector_sums[2],
        vector_sums[3],
        front_sum[:, :keys],
        front_sum[:, keys : 2 * keys],
        front_sum[:, 2 * keys : 2 * keys + values],
        front_sum[:, 2 * keys + values :],
        out_sum,
        up_sum[:, :units],
        up_sum[:, units:],
        down_sum,
    )


def solution(mesh):
    rows = P("dp", "seq", None)
    vector = P(GROUP)
    column = P(GROUP, "tensor")
    row = P("tensor", GROUP)
    return jax.shard_map(
        on_device,
        mesh=mesh,
        in_specs=(rows,)
        + (vector,) * 4
        + (column,) * 4
        + (row, column, column, row, P("tensor"), rows),
        out_specs=(rows, rows)
        + (vector,) * 4
        + (column,) * 4
        + (row, column, column, row),
        check_vma=False,
    )
```
